32 devices in a mesh: groups: 2 (over y), seq: 4 (over z), role: 2 (over x), mb: 2 (over core).
Axes of the slice: x: 2, y: 2, z: 4, core: 2. Of those that a mesh axis runs over, the one named last changes fastest.
Arguments:
- queries: bfloat16 [256, 128, 576], P(('groups', 'seq'), ('role', 'mb')), parts along dimension 0, may hold values from -200 to 200
- cache: bfloat16 [256, 256, 576], P(('groups', 'seq')), parts along dimension 0, may hold values from -24 to 24
- lengths: int32 [256], P(('groups', 'seq')), parts along dimension 0, may hold values from 2 to 256
- w_uv: bfloat16 [128, 512, 128], P(('role', 'mb'), None, 'seq'), may hold values from -0.25 to 0.25
- w_o: bfloat16 [128, 128, 3584], P(('role', 'mb'), 'seq'), may hold values from -0.1875 to 0.1875
- x_in: bfloat16 [256, 3584], P('groups', 'seq'), parts along dimension 0, may hold values from -16 to 16
- norm_gain: float32 [3584], P('seq'), may hold values from 0.1 to 1.9
- w_gate: bfloat16 [8, 3584, 2048], P(('seq', 'mb'), None, 'role'), may hold values from -0.09375 to 0.09375
- w_up: bfloat16 [8, 3584, 2048], P(('seq', 'mb'), None, 'role'), may hold values from -0.09375 to 0.09375
- w_down: bfloat16 [8, 2048, 3584], P(('seq', 'mb'), 'role'), may hold values from -0.125 to 0.125
- expert_ids: int32 [256, 2], P('groups'), parts along dimension 0, may hold values from 0 to 7, all different within a row; in each aligned block of 128 rows (0 to 127, 128 to 255, ...) at most 64 rows name the same one
- gate_weights: float32 [256, 2], P('groups'), parts along dimension 0, may hold values from 0.2 to 1
- expert_slot: int32 [8], replicated, may hold values from 0 to 7, each once
Outputs:
- layer_out: bfloat16 [256, 3584], P('groups', 'seq'), parts along dimension 0
The draws below stay inside these ranges and needn't reach their ends.
There are 2 independent parts, one for each index of `groups`. The reference program is written for one: setup_inputs(seed, part) draws one part's arguments, and reference() takes and returns one part's arrays. A program takes and returns all parts, laid end to end along the dimension named above; an argument that names none is the same for every part. Nothing has to cross between parts.
Inputs may be any that keep to these rules, and one draw needn't show every extreme that they name: `expert_ids`: each row names 2 different experts; over the rows of one group no expert is named more than 64 times, a bound that some block reaches. A permutation: expert e uses the weights at index expert_slot[e].
All inputs are finite; a program needn't handle non-finite values.
Results may differ from the reference program's by a relative error of at most 0.012.
Values may be sent and summed in bfloat16 or wider, within the bound.
No kernel may reach another device: no remote copies, remote signals or barrier semaphores. Data moves between devices by JAX's collectives and lax.ppermute only.
A program may use at most 128 MiB of HBM per device.

```python
import math
import jax
import jax.numpy as jnp
import numpy as np
from jax import lax

D = 3584
HEADS = 128
LAT = 512
ROPE = 64
VH = 128
FF = 2048
ROWS = 128
CACHE = 256
EXPERTS = 8
TOP = 2
CAP = 64


def draw_cache(key, part):
    shape = (ROWS, CACHE, LAT + ROPE)
    entries = jnp.clip(jax.random.normal(jax.random.fold_in(key, 1), shape, jnp.float32), -6.0, 6.0)
    return entries.astype(jnp.bfloat16)


def draw_queries(key, part):
    shape = (ROWS, HEADS, LAT + ROPE)
    entries = jnp.clip(jax.random.normal(jax.random.fold_in(key, 4), shape, jnp.float32), -6.0, 6.0)
    return entries.astype(jnp.bfloat16)


def draw_x_in(key, part):
    column = jnp.arange(D, dtype=jnp.float32) / (D - 1)
    base_draw = jnp.clip(jax.random.normal(jax.random.fold_in(key, 6), (ROWS, D), jnp.float32), -6.0, 6.0)
    column_scale = 3.0 ** column
    return (0.5 * base_draw * column_scale[None, :]).astype(jnp.bfloat16)


def with_ends(values, key, least, largest):
    index_at = [jax.random.randint(jax.random.fold_in(key, axis), (), 0, length) for axis, length in enumerate(values.shape)]
    main_axis = values.shape.index(max(values.shape))
    next_to = index_at[:main_axis] + [(index_at[main_axis] + 1) % values.shape[main_axis]] + index_at[main_axis + 1:]
    return values.at[tuple(index_at)].set(least).at[tuple(next_to)].set(largest)


def level_of(key, shape, cuts, least, largest):
    level, own = 1.0, jax.random.fold_in(key, 6)
    for axis_at, blocks in cuts:
        steps = jnp.exp(jax.random.uniform(jax.random.fold_in(own, axis_at), (blocks,), jnp.float32, least / len(cuts), largest / len(cuts)))
        level = level * jnp.repeat(steps, shape[axis_at] // blocks).reshape([-1 if axis == axis_at else 1 for axis in range(len(shape))])
    return level


def routed_block(rng, own, number, rows, number_of, top, bound, lean):
    order = jax.random.permutation(rng, number_of)
    crowded, usual = portions_of(number_of, rows * top, bound, lean, True), portions_of(number_of, rows * top, bound, lean, False)
    places = jnp.arange(number_of)

    def named(sizes, offset_by):
        used = int((sizes > 0).sum())
        fixed = max(1, used // 4)
        moved = fixed + (places - fixed + offset_by * (used - fixed)) % max(1, number_of - fixed)
        return jnp.zeros((number_of,), jnp.int32).at[order[jnp.where(places < fixed, places, moved)]].set(jnp.asarray(sizes, jnp.int32))

    sizes = jnp.where(number % 4 == 0, named(crowded, number // 4), named(usual, number - number // 4 - 1))
    mixed = jax.random.permutation(jax.random.fold_in(own, 3), number_of)
    giver, sink = mixed[0:number_of // 2 * 2:2], mixed[1:number_of // 2 * 2:2]
    margin = jnp.minimum(sizes[giver] - 1, bound - sizes[sink]) // 2
    margin = jnp.where((giver == order[0]) | (sink == order[0]) | (sizes[sink] == 0), 0, jnp.maximum(margin, 0))
    moved = jax.random.randint(jax.random.fold_in(own, 4), (number_of // 2,), 0, 1 << 20) % (margin + 1)
    sizes = sizes.at[giver].add(-moved).at[sink].add(moved)
    members = jnp.searchsorted(jnp.cumsum(sizes), jnp.arange(rows * top), side="right").astype(jnp.int32)
    grid = members.reshape(top, rows).T
    grid = grid[jax.random.permutation(jax.random.fold_in(own, 1), rows)]
    offset_by = jax.random.randint(jax.random.fold_in(own, 2), (rows, 1), 0, top)
    return jnp.take_along_axis(grid, (jnp.arange(top)[None, :] + offset_by) % top, axis=1)


def portions_of(number_of, total, reach, lean, full):
    weights = [(1 << 20) // math.isqrt(rank ** lean) + 1 for rank in range(1, number_of + 1)]
    largest = reach if full else min(reach, max(-(-total // number_of), total * weights[0] // sum(weights)))
    least = 1 if total - largest >= number_of - 1 else 0
    counts, surplus = [largest] + [least] * (number_of - 1), total - largest - least * (number_of - 1)
    while surplus > 0:
        candidates = [i for i in range(1, number_of) if counts[i] < largest] or [i for i in range(1, number_of) if counts[i] < reach]
        pool, budget = sum([weights[i] for i in candidates]), surplus
        for i in candidates:
            extra = min(reach - counts[i], max(1, budget * weights[i] // pool), surplus)
            counts[i] = counts[i] + extra
            surplus = surplus - extra
    return np.array(counts)


def bell_draw(rng, dims, deviation, limit, cuts=(), kind=jnp.bfloat16):
    gain = level_of(rng, dims, cuts, -0.22, 0.18) if cuts else 1.0
    values = jax.random.normal(rng, dims, jnp.float32) * deviation * gain
    return jnp.minimum(jnp.maximum(values, -limit), limit).astype(kind)


def setup_inputs(seed: int = 0, part: int = 0) -> dict:
    streams_of = jax.random.split(jax.random.key(seed), 14)
    own_keys = jax.random.split(jax.random.fold_in(streams_of[13], part), 14)
    queries = draw_queries(jax.random.fold_in(jax.random.fold_in(streams_of[13], part), 71), part)
    cache = draw_cache(jax.random.fold_in(jax.random.fold_in(streams_of[13], part), 71), part)
    lengths = with_ends(jax.random.randint(own_keys[2], (ROWS,), 2, CACHE + 1), jax.random.fold_in(own_keys[2], 1), 2, CACHE).astype(jnp.int32)
    w_uv = bell_draw(streams_of[3], (HEADS, LAT, VH), LAT ** -0.5, 0.25, ((0, 4), (2, 4)))
    w_o = bell_draw(streams_of[4], (HEADS, VH, D), (8 * VH) ** -0.5, 0.1875, ((0, 4), (1, 4)))
    x_in = draw_x_in(jax.random.fold_in(jax.random.fold_in(streams_of[13], part), 71), part)
    norm_gain = jnp.clip(1.0 + 0.18 * jax.random.normal(streams_of[6], (D,), jnp.float32), 0.1, 1.9)
    w_gate = bell_draw(streams_of[7], (EXPERTS, D, FF), D ** -0.5, 0.09375, ((0, 8), (2, 2)))
    w_up = bell_draw(streams_of[8], (EXPERTS, D, FF), D ** -0.5, 0.09375, ((0, 8), (2, 2)))
    w_down = bell_draw(streams_of[9], (EXPERTS, FF, D), FF ** -0.5, 0.125, ((0, 8), (1, 2)))
    expert_ids_keys = jax.random.split(jax.random.fold_in(own_keys[10], 1), ROWS // ROWS)
    expert_ids_turns = jax.random.permutation(jax.random.fold_in(own_keys[10], 3), ROWS // ROWS)
    expert_ids = jax.vmap(lambda own, number: routed_block(jax.random.fold_in(own_keys[10], 2), own, number, ROWS, EXPERTS, TOP, CAP, 2))(expert_ids_keys, expert_ids_turns).reshape((ROWS, TOP))
    gate_weights = jnp.clip(jax.random.uniform(own_keys[11], (ROWS, TOP), jnp.float32, 0.2, 1.0), 0.2, 1.0)
    expert_slot = jax.random.permutation(streams_of[12], EXPERTS).astype(jnp.int32)
    return dict(queries=queries, cache=cache, lengths=lengths, w_uv=w_uv, w_o=w_o, x_in=x_in, norm_gain=norm_gain, w_gate=w_gate, w_up=w_up, w_down=w_down, expert_ids=expert_ids, gate_weights=gate_weights, expert_slot=expert_slot)


def reference(queries, cache, lengths, w_uv, w_o, x_in, norm_gain, w_gate, w_up, w_down, expert_ids, gate_weights, expert_slot):
    highest = lax.Precision.HIGHEST
    score_scale = (VH + ROPE) ** (-0.5)
    scores = jnp.einsum('bhd,btd->bht', queries.astype(jnp.float32), cache.astype(jnp.float32), precision=highest) * score_scale
    positions = jnp.arange(CACHE, dtype=jnp.int32)
    valid_mask = positions[None, :] < lengths[:, None]
    scores = jnp.where(valid_mask[:, None, :], scores, -1e+30)
    row_max = lax.optimization_barrier(jnp.max(scores, axis=2, keepdims=True))
    exp_scores = jnp.where(valid_mask[:, None, :], jnp.exp(scores - row_max), 0.0)
    denominator = lax.optimization_barrier(jnp.sum(exp_scores, axis=2))
    probs = exp_scores.astype(jnp.bfloat16)
    numerator = jnp.einsum('bht,btc->bhc', probs.astype(jnp.float32), cache[:, :, :LAT].astype(jnp.float32), precision=highest)
    latent = (numerator / denominator[:, :, None]).astype(jnp.bfloat16)
    values = jnp.einsum('bhc,hcj->bhj', latent.astype(jnp.float32), w_uv.astype(jnp.float32), precision=highest).astype(jnp.bfloat16)
    attention = jnp.einsum('bhj,hjd->bd', values.astype(jnp.float32), w_o.astype(jnp.float32), precision=highest)
    hidden = x_in.astype(jnp.float32) + attention
    mean_square = lax.optimization_barrier(jnp.mean(hidden * hidden, axis=1, keepdims=True))
    normed = (hidden * lax.rsqrt(mean_square + 1e-06) * norm_gain).astype(jnp.bfloat16)
    expert_range = jnp.arange(EXPERTS, dtype=jnp.int32)
    coefficients = lax.optimization_barrier(jnp.sum(jnp.where(expert_ids[:, :, None] == expert_range[None, None, :], gate_weights[:, :, None], 0.0), axis=1))

    def expert_out(expert):
        slot_index = expert_slot[expert]
        gate_out = jnp.dot(normed, w_gate[slot_index], preferred_element_type=jnp.float32)
        up_out = jnp.dot(normed, w_up[slot_index], preferred_element_type=jnp.float32)
        activated = (jax.nn.silu(gate_out) * up_out).astype(jnp.bfloat16)
        return jnp.dot(activated, w_down[slot_index], preferred_element_type=jnp.float32)
    outputs = lax.map(expert_out, expert_range)
    mixture = jnp.einsum('be,ebd->bd', coefficients, outputs, precision=highest)
    return (hidden + mixture).astype(jnp.bfloat16)
```

```python
import jax
import jax.numpy as jnp
from jax import lax
from jax.sharding import PartitionSpec as P

CAP = 64
EPS = 1e-06
BF = jnp.bfloat16
F32 = jnp.float32


def swap(value, axis, offset):
    count = lax.axis_size(axis)
    return lax.ppermute(value, axis, [(i, i ^ offset) for i in range(count)])


def block(value, index, axis=0):
    return lax.dynamic_index_in_dim(value, index, axis, keepdims=False)


def in_order(parts, me):
    return jnp.stack([lax.select_n(me ^ s, *parts) if len(parts) > 2
                      else jnp.where((me ^ s) == 0, parts[0], parts[1])
                      for s in range(len(parts))])


def sum_scatter(value, axis):
    me, count = lax.axis_index(axis), lax.axis_size(axis)
    sent = [swap(block(value, me ^ k).astype(BF), axis, k) for k in range(1, count)]
    total = block(value, me)
    for part in sent:
        total = total + part.astype(F32)
    return total


def gather_parts(value, axis):
    return [value] + [swap(value, axis, k) for k in range(1, lax.axis_size(axis))]


def attend(queries, cache, lengths, latent_width, score_scale):
    positions = jnp.arange(cache.shape[1], dtype=jnp.int32)
    valid = positions[None, :] < lengths[:, None]
    scores = jnp.einsum("bhd,btd->bht", queries, cache, preferred_element_type=F32) * score_scale
    scores = jnp.where(valid[:, None, :], scores, -1e30)
    row_max = jnp.max(scores, axis=2)
    exp_scores = jnp.where(valid[:, None, :], jnp.exp(scores - row_max[:, :, None]), 0.0)
    denominator = jnp.sum(exp_scores, axis=2)
    numerator = jnp.einsum(
        "bht,btc->bhc", exp_scores.astype(BF), cache[:, :, :latent_width], preferred_element_type=F32
    )
    return (numerator / denominator[:, :, None]).astype(BF)


def per_device(
    queries, cache, lengths, w_uv, w_o, x_in, norm_gain, w_gate, w_up, w_down,
    expert_ids, gate_weights, expert_slot,
):
    groups, seqs = lax.axis_size("groups"), lax.axis_size("seq")
    roles, cores = lax.axis_size("role"), lax.axis_size("mb")
    g, z = lax.axis_index("groups"), lax.axis_index("seq")
    x, c = lax.axis_index("role"), lax.axis_index("mb")
    heads, latent_width, width = w_uv.shape
    own_rows = queries.shape[0]
    rows, feats = x_in.shape
    model = feats * seqs
    near = 1
    while near * near < seqs:
        near *= 2
    far = seqs // near

    part = block(w_uv.reshape(groups, heads // groups, latent_width, width), g)
    foreign_maps = []
    for k in range(1, far):
        fetched = swap(part, "seq", k * near)
        both = in_order(gather_parts(fetched, "groups"), g)
        foreign_maps.append(both.reshape(heads, latent_width, width))

    score_scale = (width * seqs + queries.shape[2] - latent_width) ** (-0.5)
    latent = attend(queries, cache, lengths, latent_width, score_scale)
    latents = jnp.stack([latent] + [swap(latent, "seq", k) for k in range(1, near)])
    latents = latents.reshape(near * own_rows, heads, latent_width)

    def project(value_map):
        return jnp.einsum("bhc,hcj->bhj", latents, value_map, preferred_element_type=F32).astype(BF)

    given = [swap(project(m), "seq", (k + 1) * near) for k, m in enumerate(foreign_maps)]
    pieces = []
    for value in [project(w_uv)] + given:
        value = value.reshape(near, own_rows, heads * width)
        pieces += [value[i] for i in range(near)]
    values = in_order(pieces, z).reshape(rows, heads * width)
    attn = jnp.dot(values, w_o.reshape(heads * width, model), preferred_element_type=F32)

    quarter = rows // (roles * cores)
    attn = attn.reshape(roles, cores, quarter, model).transpose(1, 0, 2, 3)
    attn = sum_scatter(attn, "mb")
    attn = sum_scatter(attn, "role")
    attn = sum_scatter(attn.reshape(quarter, seqs, feats).transpose(1, 0, 2), "seq")
    x_own = block(x_in.reshape(roles * cores, quarter, feats), x * cores + c)
    hidden = x_own.astype(F32) + attn

    squares = jnp.sum(hidden * hidden, axis=1, keepdims=True)
    high = squares.astype(BF)
    low = (squares - high.astype(F32)).astype(BF)
    pad = jnp.zeros((quarter, 126), BF)
    packed = jnp.concatenate([(hidden * norm_gain[None, :]).astype(BF), high, low, pad], axis=1)
    parts = gather_parts(packed, "seq")
    total = sum(p[:, feats].astype(F32) + p[:, feats + 1].astype(F32) for p in parts)
    scale = lax.rsqrt(total / model + EPS)
    ordered = in_order([p[:, :feats] for p in parts], z)
    normed = (ordered.astype(F32) * scale[None, :, None]).astype(BF)
    normed = normed.transpose(1, 0, 2).reshape(quarter, model)
    normed = jnp.stack(gather_parts(normed, "role"))
    normed = jnp.stack(gather_parts(normed, "mb"))

    experts = expert_slot.shape[0]
    slot = z * cores + c
    mine_slot = jnp.sum(
        jnp.where(expert_ids[:, :, None] == jnp.arange(experts, dtype=jnp.int32), expert_slot, 0), axis=2
    ) == slot
    member = jnp.any(mine_slot, axis=1)
    gate_row = jnp.sum(jnp.where(mine_slot, gate_weights, 0.0), axis=1)
    lower = (jnp.arange(rows)[:, None] > jnp.arange(rows)[None, :]).astype(F32)
    position = jnp.dot(lower, member.astype(F32)[:, None])[:, 0].astype(jnp.int32)
    select = member[None, :] & (position[None, :] == jnp.arange(CAP, dtype=jnp.int32)[:, None])
    slot_gate = jnp.sum(jnp.where(select, gate_row[None, :], 0.0), axis=1, keepdims=True)
    blocks = select.reshape(CAP, roles, cores, quarter)
    picker = jnp.stack([
        jnp.stack([block(block(blocks, c ^ j, 2), x ^ i, 1) for i in range(roles)], axis=1)
        for j in range(cores)
    ], axis=1).reshape(CAP, rows).astype(BF)

    picked = jnp.dot(picker, normed.reshape(rows, model), preferred_element_type=F32).astype(BF)
    gate_out = jnp.dot(picked, w_gate[0], preferred_element_type=F32)
    up_out = jnp.dot(picked, w_up[0], preferred_element_type=F32)
    activated = (jax.nn.silu(gate_out) * up_out).astype(BF)
    result = jnp.dot(activated, w_down[0], preferred_element_type=F32)
    result = (result * slot_gate).astype(BF)

    spread = blocks.transpose(2, 1, 3, 0).reshape(cores, roles * quarter, CAP).astype(BF)
    sent = [
        swap(jnp.dot(block(spread, c ^ k), result, preferred_element_type=F32).astype(BF), "mb", k)
        for k in range(1, cores)
    ]
    mixed = jnp.dot(block(spread, c), result, preferred_element_type=F32)
    for p in sent:
        mixed = mixed + p.astype(F32)
    mixed = sum_scatter(mixed.reshape(roles * quarter, seqs, feats).transpose(1, 0, 2), "seq")
    mixed = mixed.reshape(roles, quarter, feats)
    at_own = jnp.arange(roles)[:, None, None] == x
    mixed = jnp.where(at_own, mixed + hidden[None], mixed).astype(BF)
    shares = gather_parts(mixed, "role")
    shares = shares if roles == 2 else in_order(shares, x)
    out = sum(p.astype(F32) for p in shares).astype(BF)
    out = in_order(gather_parts(out, "mb"), c)
    return out.transpose(1, 0, 2, 3).reshape(rows, feats)


def solution(mesh):
    in_specs = (
        P(("groups", "seq"), ("role", "mb"), None),
        P(("groups", "seq"), None, None),
        P(("groups", "seq")),
        P(("role", "mb"), None, "seq"),
        P(("role", "mb"), "seq", None),
        P("groups", "seq"),
        P("seq"),
        P(("seq", "mb"), None, "role"),
        P(("seq", "mb"), None, "role"),
        P(("seq", "mb"), "role", None),
        P("groups", None),
        P("groups", None),
        P(),
    )
    out_specs = P("groups", "seq")
    return jax.shard_map(
        per_device, mesh=mesh, in_specs=in_specs, out_specs=out_specs, check_vma=False
    )
```
